32 devices in a mesh: rep: 1 (over z), dp: 32 (over x, y, core).
Axes of the slice: x: 4, y: 4, z: 1, core: 2. Of those that a mesh axis runs over, the one named last changes fastest.
The devices are a block of a 4x4x8 slice.
Arguments:
- g_w_gate: bfloat16 [32, 2, 1152, 4608], P(('rep', 'dp'))
- g_w_up: bfloat16 [32, 2, 1152, 4608], P(('rep', 'dp'))
- g_w_down: bfloat16 [32, 2, 4608, 1152], P(('rep', 'dp'))
- w_gate: bfloat16 [2, 1152, 4608], replicated
- w_up: bfloat16 [2, 1152, 4608], replicated
- w_down: bfloat16 [2, 4608, 1152], replicated
- m_w_gate: float32 [2, 1152, 4608], P(None, 'dp')
- m_w_up: float32 [2, 1152, 4608], P(None, 'dp')
- m_w_down: float32 [2, 4608, 1152], P(None, 'dp')
- v_w_gate: float32 [2, 1152, 4608], P(None, 'dp')
- v_w_up: float32 [2, 1152, 4608], P(None, 'dp')
- v_w_down: float32 [2, 4608, 1152], P(None, 'dp')
Outputs:
- output 1: bfloat16 [2, 1152, 4608], P('rep')
- output 2: bfloat16 [2, 1152, 4608], P('rep')
- output 3: bfloat16 [2, 4608, 1152], P('rep')
- output 4: float32 [2, 1152, 4608], P('rep', 'dp')
- output 5: float32 [2, 1152, 4608], P('rep', 'dp')
- output 6: float32 [2, 4608, 1152], P('rep', 'dp')
- output 7: float32 [2, 1152, 4608], P('rep', 'dp')
- output 8: float32 [2, 1152, 4608], P('rep', 'dp')
- output 9: float32 [2, 4608, 1152], P('rep', 'dp')
All inputs are finite; a program needn't handle non-finite values.
Results may differ from the reference program's by a relative error of at most 0.022.
Values are sent between devices in bfloat16 or wider.
A program may use at most 768 MiB of HBM per device.

```python
import jax
import jax.numpy as jnp
from jax import lax

DEVICES = 32
D = 1152
FF = 4608
LAYERS = 2
NAMES = ("w_gate", "w_up", "w_down")
SHAPES = {"w_gate": (LAYERS, D, FF), "w_up": (LAYERS, D, FF), "w_down": (LAYERS, FF, D)}


def setup_inputs(seed: int = 0, part: int = 0) -> dict:
    kz, *keys = jax.random.split(jax.random.key(seed), 1 + 5 * len(NAMES))
    loud = 2.0 ** jax.random.uniform(kz, (), jnp.float32, -1.0, 1.0)
    drawn = {}
    for name, key, both in zip(NAMES, keys[:3], keys[3:6], strict=True):
        own = jax.random.normal(jax.random.fold_in(key, part), (DEVICES, *SHAPES[name]), jnp.float32)
        shared = jax.random.normal(jax.random.fold_in(both, part), SHAPES[name], jnp.float32)
        drawn["g_" + name] = (loud * (0.7 * shared / DEVICES + 0.7 * own * DEVICES**-0.5)).astype(jnp.bfloat16)
    for name, key in zip(NAMES, keys[6:9], strict=True):
        drawn[name] = (jax.random.normal(key, SHAPES[name], jnp.float32) * SHAPES[name][1] ** -0.5).astype(jnp.bfloat16)
    for name, key in zip(NAMES, keys[9:12], strict=True):
        drawn["m_" + name] = loud * 0.5 * jax.random.normal(key, SHAPES[name], jnp.float32)
    for name, key in zip(NAMES, keys[12:15], strict=True):
        drawn["v_" + name] = loud * loud * jax.random.uniform(key, SHAPES[name], jnp.float32, 0.5, 1.5)
    return drawn


def adamw(w, m, v, g):
    m = 0.9 * m + 0.1 * g
    v = 0.95 * v + 0.05 * g * g
    step = m * lax.rsqrt(v + 1e-8) + 0.1 * w
    return (w - 0.02 * step).astype(jnp.bfloat16), m, v


def reference(g_w_gate, g_w_up, g_w_down, w_gate, w_up, w_down, m_w_gate, m_w_up, m_w_down, v_w_gate, v_w_up, v_w_down):
    def total(terms):
        return lax.scan(lambda so_far, term: (so_far + term.astype(jnp.float32), None), jnp.zeros(terms.shape[1:], jnp.float32), terms)[0]

    gradients = [total(terms).astype(jnp.bfloat16).astype(jnp.float32) for terms in (g_w_gate, g_w_up, g_w_down)]
    new = [
        adamw(w.astype(jnp.float32), m, v, g)
        for w, m, v, g in zip((w_gate, w_up, w_down), (m_w_gate, m_w_up, m_w_down), (v_w_gate, v_w_up, v_w_down), gradients, strict=True)
    ]
    return tuple(one[which] for which in range(3) for one in new)
```

```python
import functools
import math

import jax
import jax.numpy as jnp
from jax import lax
from jax.experimental import pallas as pl
from jax.experimental.pallas import tpu as pltpu
from jax.sharding import PartitionSpec as P

MESH = pl.DeviceIdType.MESH
F32, BF16 = jnp.float32, jnp.bfloat16
SLOTS = 4
HOLD = 3


def adamw(w, m, v, g):
    m = 0.9 * m + 0.1 * g
    v = 0.95 * v + 0.05 * g * g
    step = m * lax.rsqrt(v + 1e-8) + 0.1 * w
    return (w - 0.02 * step).astype(BF16), m, v


class Place:
    def __init__(self, side):
        me = lax.axis_index("dp")
        self.side = side
        self.core = me % 2
        chip = me // 2
        x, y = chip // side, chip % side
        self.chip = chip
        self.f = x + self.core * (y - x)
        self.s = y + self.core * (x - y)
        self.mf = side - (side - 1) * self.core
        self.ms = 1 + (side - 1) * self.core

    def device(self, df, ds):
        f, s = (self.f + df) % self.side, (self.s + ds) % self.side
        return {"dp": (f * self.mf + s * self.ms) * 2 + self.core}

    def partner(self):
        return {"dp": self.chip * 2 + 1 - self.core}

    def around(self):
        d = self.side - 1
        return [self.device(1, 0), self.device(d, 0), self.device(0, 1), self.device(0, d), self.partner()]

    def greet(self):
        barrier = pltpu.get_barrier_semaphore()
        others = self.around()
        for other in others:
            pl.semaphore_signal(barrier, inc=1, device_id=other, device_id_type=MESH)
        pl.semaphore_wait(barrier, len(others))


def send(src, dst, send_sem, recv_sem, device):
    return pltpu.make_async_remote_copy(
        src_ref=src, dst_ref=dst, send_sem=send_sem, recv_sem=recv_sem, device_id=device, device_id_type=MESH
    )


def wait_for(ref, sem):
    pltpu.make_async_copy(ref, ref, sem).wait()


def reduce_kernel(side, quarters, rows, cols, *refs):
    terms = refs[:3]
    out = refs[3]
    (own, par, ra, rb, fl, fr, hold, sums, ra2, rb2, fl2, fr2, g) = refs[4:17]
    (own_sem, par_send, par_sem, a_send, ra_sem, rb_sem, fl_sem, fr_sem, s_send, ra2_sem, rb2_sem, fl2_sem, fr2_sem, g_send, g_sem, out_sem, credit) = refs[17:]
    pieces = 3 * quarters
    half = side // 2
    top = (rows // 2 + 7) // 8 * 8
    at = Place(side)
    core, f, s = at.core, at.f, at.s
    last = side - 1
    right, left = at.device(1, 0), at.device(last, 0)
    up, down = at.device(0, 1), at.device(0, last)
    partner = at.partner()
    fp, fm, f2 = (f + 1) % side, (f + last) % side, (f + 2) % side
    sp, sm, s2 = (s + 1) % side, (s + last) % side, (s + 2) % side
    at.greet()

    def block(which, layer, quarter, chip):
        ref = terms[which]
        if which < 2:
            return ref.at[0, layer, pl.ds(pl.multiple_of(chip * rows, 8), rows), pl.ds(pl.multiple_of(quarter * cols, 128), cols)]
        return ref.at[0, layer, pl.ds(pl.multiple_of((chip * quarters + quarter) * rows, 8), rows), :]

    def load(i):
        slot = i % SLOTS
        for which in range(3):

            @pl.when(i // quarters == which)
            def _(which=which):
                @pl.loop(0, side * side)
                def _(n):
                    bf, bs = n // side, n % side
                    send(
                        block(which, 1 - core, i % quarters, bf * at.ms + bs * at.mf),
                        par.at[slot, bf, bs],
                        par_send.at[slot],
                        par_sem.at[slot],
                        partner,
                    ).start()
                    pltpu.make_async_copy(
                        block(which, core, i % quarters, bf * at.mf + bs * at.ms), own.at[slot, bf, bs], own_sem.at[slot]
                    ).start()

    def pair(slot, bf, bs):
        return own[slot, bf, bs].astype(F32) + par[slot, bf, bs].astype(F32)

    load(0)
    load(1)

    @pl.loop(0, pieces + 4)
    def _(t):
        @pl.when(t < pieces)
        def _():
            i, slot = t, t % SLOTS
            wait_for(own.at[slot], own_sem.at[slot])
            wait_for(par.at[slot], par_sem.at[slot])

            @pl.loop(0, side)
            def _(n):
                own[slot, f2, n] = pair(slot, f2, n).astype(BF16)

            send(own.at[slot, f2, pl.ds(0, half)], ra.at[i], a_send.at[slot], ra_sem.at[i], right).start()
            send(own.at[slot, f2, pl.ds(half, half)], rb.at[i], a_send.at[slot], rb_sem.at[i], left).start()

            @pl.loop(0, half)
            def _(n):
                own[slot, fp, half + n] = pair(slot, fp, half + n).astype(BF16)
                own[slot, fm, n] = pair(slot, fm, n).astype(BF16)

            send(own.at[slot, fp, pl.ds(half, half)], fl.at[i, pl.ds(half, half)], a_send.at[slot], fl_sem.at[i], right).start()
            send(own.at[slot, fm, pl.ds(0, half)], fr.at[i, pl.ds(0, half)], a_send.at[slot], fr_sem.at[i], left).start()

        @pl.when((t >= 1) & (t < pieces + 1))
        def _():
            i = t - 1
            slot = i % SLOTS
            wait_for(ra.at[i], ra_sem.at[i])
            wait_for(rb.at[i], rb_sem.at[i])

            @pl.loop(0, half)
            def _(n):
                own[slot, fp, n] = (pair(slot, fp, n) + ra[i, n].astype(F32)).astype(BF16)
                own[slot, fm, half + n] = (pair(slot, fm, half + n) + rb[i, n].astype(F32)).astype(BF16)

            send(own.at[slot, fp, pl.ds(0, half)], fl.at[i, pl.ds(0, half)], a_send.at[slot], fl_sem.at[i], right).start()
            send(own.at[slot, fm, pl.ds(half, half)], fr.at[i, pl.ds(half, half)], a_send.at[slot], fr_sem.at[i], left).start()

        @pl.when((t >= 2) & (t < pieces + 2))
        def _():
            i = t - 2
            slot, h = i % SLOTS, i % HOLD

            @pl.when(i >= HOLD)
            def _():
                wait_for(sums.at[h, pl.ds(0, last)], s_send.at[h])

            wait_for(fl.at[i], fl_sem.at[i])
            wait_for(fr.at[i], fr_sem.at[i])

            @pl.loop(0, side)
            def _(n):
                total = pair(slot, f, n) + fl[i, n].astype(F32) + fr[i, n].astype(F32)
                hold[h, n] = total
                sums[h, n] = total.astype(BF16)

            send(sums.at[h, s2, pl.ds(0, top)], ra2.at[i], s_send.at[h], ra2_sem.at[i], up).start()
            send(sums.at[h, s2, pl.ds(top, rows - top)], rb2.at[i], s_send.at[h], rb2_sem.at[i], down).start()
            send(sums.at[h, sp, pl.ds(top, rows - top)], fl2.at[i, pl.ds(top, rows - top)], s_send.at[h], fl2_sem.at[i], up).start()
            send(sums.at[h, sm, pl.ds(0, top)], fr2.at[i, pl.ds(0, top)], s_send.at[h], fr2_sem.at[i], down).start()

            @pl.when(i + SLOTS < pieces)
            def _():
                pl.semaphore_signal(credit, inc=1, device_id=partner, device_id_type=MESH)

        @pl.when(t + 2 < pieces)
        def _():
            @pl.when(t + 2 >= SLOTS)
            def _():
                slot = (t + 2) % SLOTS
                wait_for(own.at[slot, pl.ds(0, last)], a_send.at[slot])
                wait_for(own.at[slot], par_send.at[slot])
                pl.semaphore_wait(credit, 1)

            load(t + 2)

        @pl.when((t >= 3) & (t < pieces + 3))
        def _():
            i = t - 3
            h = i % HOLD
            wait_for(ra2.at[i], ra2_sem.at[i])
            wait_for(rb2.at[i], rb2_sem.at[i])
            sums[h, sp, pl.ds(0, top)] = (hold[h, sp, pl.ds(0, top)] + ra2[i].astype(F32)).astype(BF16)
            sums[h, sm, pl.ds(top, rows - top)] = (hold[h, sm, pl.ds(top, rows - top)] + rb2[i].astype(F32)).astype(BF16)
            send(sums.at[h, sp, pl.ds(0, top)], fl2.at[i, pl.ds(0, top)], s_send.at[h], fl2_sem.at[i], up).start()
            send(sums.at[h, sm, pl.ds(top, rows - top)], fr2.at[i, pl.ds(top, rows - top)], s_send.at[h], fr2_sem.at[i], down).start()

        @pl.when(t >= 4)
        def _():
            i = t - 4
            h = i % HOLD
            wait_for(fl2.at[i], fl2_sem.at[i])
            wait_for(fr2.at[i], fr2_sem.at[i])
            g[i, core] = (hold[h, s] + fl2[i].astype(F32) + fr2[i].astype(F32)).astype(BF16)
            send(g.at[i, core], g.at[i, core], g_send.at[i], g_sem.at[i], partner).start()

    @pl.loop(0, pieces)
    def _(i):
        wait_for(g.at[i, core], g_sem.at[i])
        pltpu.make_async_copy(g.at[i], out.at[i], out_sem.at[i]).start()

    for n in range(SLOTS):
        slot = (pieces + n) % SLOTS
        wait_for(own.at[slot, pl.ds(0, last)], a_send.at[slot])
        wait_for(own.at[slot], par_send.at[slot])
    for n in range(HOLD):
        wait_for(sums.at[n, pl.ds(0, last)], s_send.at[n])

    @pl.loop(0, pieces)
    def _(i):
        wait_for(g.at[i, core], g_send.at[i])
        pltpu.make_async_copy(g.at[i], out.at[i], out_sem.at[i]).wait()


def reduce_scatter(terms, side):
    _, layers, d, ff = terms[0].shape
    quarters = ff // d
    rows, cols = d // (side * side), d
    pieces = 3 * quarters
    if side != 4 or layers != 2:
        raise ValueError("wrong sizes")
    top = (rows // 2 + 7) // 8 * 8
    dma = pltpu.SemaphoreType.DMA
    any_ = pl.BlockSpec(memory_space=pl.ANY)
    return pl.pallas_call(
        functools.partial(reduce_kernel, side, quarters, rows, cols),
        out_shape=jax.ShapeDtypeStruct((pieces, layers, rows, cols), BF16),
        in_specs=[any_] * 3,
        out_specs=any_,
        scratch_shapes=[
            pltpu.VMEM((SLOTS, side, side, rows, cols), BF16),
            pltpu.VMEM((SLOTS, side, side, rows, cols), BF16),
            pltpu.VMEM((pieces, side // 2, rows, cols), BF16),
            pltpu.VMEM((pieces, side // 2, rows, cols), BF16),
            pltpu.VMEM((pieces, side, rows, cols), BF16),
            pltpu.VMEM((pieces, side, rows, cols), BF16),
            pltpu.VMEM((HOLD, side, rows, cols), F32),
            pltpu.VMEM((HOLD, side, rows, cols), BF16),
            pltpu.VMEM((pieces, top, cols), BF16),
            pltpu.VMEM((pieces, rows - top, cols), BF16),
            pltpu.VMEM((pieces, rows, cols), BF16),
            pltpu.VMEM((pieces, rows, cols), BF16),
            pltpu.VMEM((pieces, layers, rows, cols), BF16),
            dma((SLOTS,)),
            dma((SLOTS,)),
            dma((SLOTS,)),
            dma((SLOTS,)),
            dma((pieces,)),
            dma((pieces,)),
            dma((pieces,)),
            dma((pieces,)),
            dma((HOLD,)),
            dma((pieces,)),
            dma((pieces,)),
            dma((pieces,)),
            dma((pieces,)),
            dma((pieces,)),
            dma((pieces,)),
            dma((pieces,)),
            pltpu.SemaphoreType.REGULAR,
        ],
        compiler_params=pltpu.CompilerParams(collective_id=0, has_side_effects=True, vmem_limit_bytes=67043328),
        name="reduce_scatter",
    )(*terms)


def solution(mesh):
    side = math.isqrt(mesh.shape["dp"] // 2)

    def step(*arrays):
        terms, weights, m, v = (arrays[i : i + 3] for i in (0, 3, 6, 9))
        me = lax.axis_index("dp")
        quarters = terms[0].shape[3] // terms[0].shape[2]
        pieces = reduce_scatter(terms, side)
        gradients = []
        for n in range(3):
            part = pieces[n * quarters : (n + 1) * quarters]
            part = part.transpose(1, 2, 0, 3) if n < 2 else part.transpose(1, 0, 2, 3)
            part = part.reshape(part.shape[0], -1, weights[n].shape[2])
            own = m[n].shape[1]
            gradients.append(lax.dynamic_slice_in_dim(part, me % 2 * own, own, 1).astype(F32))
        own = [lax.dynamic_slice_in_dim(w, me * one.shape[1], one.shape[1], 1).astype(F32) for w, one in zip(weights, m, strict=True)]
        new = [adamw(w, m, v, g) for w, m, v, g in zip(own, m, v, gradients, strict=True)]
        whole = [lax.all_gather(one[0], "dp", axis=1, tiled=True) for one in new]
        return (*whole, *(one[1] for one in new), *(one[2] for one in new))

    all_of, cut = P(None, None, None), P(None, "dp", None)
    return jax.shard_map(
        step,
        mesh=mesh,
        in_specs=(P(("rep", "dp"), None, None, None),) * 3 + (all_of,) * 3 + (cut,) * 6,
        out_specs=(P("rep", None, None),) * 3 + (P("rep", "dp", None),) * 6,
        check_vma=False,
    )
```

```python
import functools
import math

import jax
import jax.numpy as jnp
from jax import lax
from jax.experimental import pallas as pl
from jax.experimental.pallas import tpu as pltpu
from jax.sharding import PartitionSpec as P


MESH = pl.DeviceIdType.MESH
F32, BF16 = jnp.float32, jnp.bfloat16
SLOTS = 4
HOLD = 3
RING_A, RING_F = 4, 6


def adamw(w, m, v, g):
    m = 0.9 * m + 0.1 * g
    v = 0.95 * v + 0.05 * g * g
    step = m * lax.rsqrt(v + 1e-8) + 0.1 * w
    return (w - 0.02 * step).astype(BF16), m, v


class Place:
    def __init__(self, side):
        me = lax.axis_index("dp")
        self.side = side
        self.core = me % 2
        chip = me // 2
        x, y = chip // side, chip % side
        self.chip = chip
        self.f = x + self.core * (y - x)
        self.s = y + self.core * (x - y)
        self.mf = side - (side - 1) * self.core
        self.ms = 1 + (side - 1) * self.core

    def device(self, df, ds):
        f, s = (self.f + df) % self.side, (self.s + ds) % self.side
        return {"dp": (f * self.mf + s * self.ms) * 2 + self.core}

    def partner(self):
        return {"dp": self.chip * 2 + 1 - self.core}

    def around(self):
        d = self.side - 1
        return [self.device(1, 0), self.device(d, 0), self.device(0, 1), self.device(0, d), self.partner()]

    def greet(self):
        barrier = pltpu.get_barrier_semaphore()
        others = self.around()
        for other in others:
            pl.semaphore_signal(barrier, inc=1, device_id=other, device_id_type=MESH)
        pl.semaphore_wait(barrier, len(others))


def send(src, dst, send_sem, recv_sem, device):
    return pltpu.make_async_remote_copy(
        src_ref=src, dst_ref=dst, send_sem=send_sem, recv_sem=recv_sem, device_id=device, device_id_type=MESH
    )


def wait_for(ref, sem):
    pltpu.make_async_copy(ref, ref, sem).wait()


def reduce_kernel(side, quarters, rows, cols, *refs):
    terms, weights, ms, vs = (refs[n : n + 3] for n in (0, 3, 6, 9))
    out, units = refs[12], refs[13:17]
    (own, par, ra, rb, fl, fr, hold, sums, ra2, rb2, fl2, fr2, g, mv_own, mv_par, mv_down, w_old, w_new) = refs[17:35]
    (own_sem, par_send, par_sem, a_send, ra_sem, rb_sem, fl_sem, fr_sem, s_send, ra2_sem, rb2_sem, fl2_sem, fr2_sem, g_send, g_sem, out_sem) = refs[35:51]
    (w_sem, mv_sem, mp_sem, mp_send, n_send, n_own, nl_sem, nr_sem, no_sem, f_send, credit) = refs[51:]
    pieces = 3 * quarters
    wide = 2 * quarters
    half = side // 2
    top = (rows // 2 + 7) // 8 * 8
    at = Place(side)
    core, f, s = at.core, at.f, at.s
    last = side - 1
    right, left = at.device(1, 0), at.device(last, 0)
    up, down = at.device(0, 1), at.device(0, last)
    partner = at.partner()
    fp, fm, f2 = (f + 1) % side, (f + last) % side, (f + 2) % side
    sp, sm, s2 = (s + 1) % side, (s + last) % side, (s + 2) % side
    at.greet()

    def columns(quarter):
        return pl.ds(pl.multiple_of(quarter * cols, 128), cols)

    def block(refs, which, lead, layer, quarter, chip):
        ref = refs[which]
        if which < 2:
            return ref.at[*lead, layer, pl.ds(pl.multiple_of(chip * rows, 8), rows), columns(quarter)]
        return ref.at[*lead, layer, pl.ds(pl.multiple_of((chip * quarters + quarter) * rows, 8), rows), :]

    def each(i, do):
        for which in range(3):

            @pl.when(i // quarters == which)
            def _(which=which):
                do(which, i % quarters)

    def load(i):
        slot = i % SLOTS

        def do(which, quarter):
            @pl.loop(0, side * side)
            def _(n):
                bf, bs = n // side, n % side
                send(
                    block(terms, which, (0,), 1 - core, quarter, bf * at.ms + bs * at.mf),
                    par.at[slot, bf, bs],
                    par_send.at[slot],
                    par_sem.at[slot],
                    partner,
                ).start()
                pltpu.make_async_copy(
                    block(terms, which, (0,), core, quarter, bf * at.mf + bs * at.ms), own.at[slot, bf, bs], own_sem.at[slot]
                ).start()

        each(i, do)

    def load_state(i):
        def do(which, quarter):
            pltpu.make_async_copy(block(weights, which, (), core, quarter, at.chip), w_old.at[i], w_sem.at[i]).start()
            for n, ref in enumerate((ms[which], vs[which])):
                if which < 2:
                    part = ref.at[:, :, columns(quarter)]
                    pltpu.make_async_copy(part, mv_own.at[i, n], mv_sem.at[i]).start()
                    send(part, mv_par.at[i, n], mp_send.at[i], mp_sem.at[i], partner).start()
                else:

                    @pl.when(quarter // half == core)
                    def _(n=n, ref=ref):
                        here = pl.ds(pl.multiple_of(quarter % half * rows, 8), rows)
                        pltpu.make_async_copy(ref.at[core, here], mv_down.at[quarter, n], mv_sem.at[i]).start()
                        send(ref.at[1 - core, here], mv_down.at[quarter, n], mp_send.at[i], mp_sem.at[i], partner).start()

        each(i, do)

    def unit(i, do):
        for n in range(2):

            @pl.when(i // quarters == n)
            def _(n=n):
                do(lambda bf, at_row, size: units[n].at[bf, pl.ds(at_row, size), columns(i % quarters)])

        for n in range(2):

            @pl.when((i >= wide) & ((i - wide) // half == n))
            def _(n=n):
                start = pl.multiple_of(i % half * rows, 8)
                do(lambda bf, at_row, size: units[2 + n].at[bf, pl.ds(start + at_row, size), :])

    def pair(slot, bf, bs):
        return own[slot, bf, bs].astype(F32) + par[slot, bf, bs].astype(F32)

    load(0)
    load(1)

    @pl.loop(0, pieces + 5)
    def _(t):
        @pl.when(t < pieces)
        def _():
            i, slot = t, t % SLOTS
            a, b = i % RING_A, i % RING_F
            wait_for(own.at[slot], own_sem.at[slot])
            wait_for(par.at[slot], par_sem.at[slot])

            @pl.loop(0, side)
            def _(n):
                own[slot, f2, n] = pair(slot, f2, n).astype(BF16)

            send(own.at[slot, f2, pl.ds(0, half)], ra.at[a], a_send.at[slot], ra_sem.at[a], right).start()
            send(own.at[slot, f2, pl.ds(half, half)], rb.at[a], a_send.at[slot], rb_sem.at[a], left).start()

            @pl.loop(0, half)
            def _(n):
                own[slot, fp, half + n] = pair(slot, fp, half + n).astype(BF16)
                own[slot, fm, n] = pair(slot, fm, n).astype(BF16)

            send(own.at[slot, fp, pl.ds(half, half)], fl.at[b, pl.ds(half, half)], a_send.at[slot], fl_sem.at[b], right).start()
            send(own.at[slot, fm, pl.ds(0, half)], fr.at[b, pl.ds(0, half)], a_send.at[slot], fr_sem.at[b], left).start()

        @pl.when((t >= 1) & (t < pieces + 1))
        def _():
            i = t - 1
            slot, a, b = i % SLOTS, i % RING_A, i % RING_F
            wait_for(ra.at[a], ra_sem.at[a])
            wait_for(rb.at[a], rb_sem.at[a])

            @pl.loop(0, half)
            def _(n):
                own[slot, fp, n] = (pair(slot, fp, n) + ra[a, n].astype(F32)).astype(BF16)
                own[slot, fm, half + n] = (pair(slot, fm, half + n) + rb[a, n].astype(F32)).astype(BF16)

            send(own.at[slot, fp, pl.ds(0, half)], fl.at[b, pl.ds(0, half)], a_send.at[slot], fl_sem.at[b], right).start()
            send(own.at[slot, fm, pl.ds(half, half)], fr.at[b, pl.ds(half, half)], a_send.at[slot], fr_sem.at[b], left).start()

        @pl.when((t >= 2) & (t < pieces + 2))
        def _():
            i = t - 2
            slot, h, a, b = i % SLOTS, i % HOLD, i % RING_A, i % RING_F

            @pl.when(i >= HOLD)
            def _():
                wait_for(sums.at[h, pl.ds(0, last)], s_send.at[h])

            wait_for(fl.at[b], fl_sem.at[b])
            wait_for(fr.at[b], fr_sem.at[b])

            @pl.loop(0, side)
            def _(n):
                total = pair(slot, f, n) + fl[b, n].astype(F32) + fr[b, n].astype(F32)
                hold[h, n] = total
                sums[h, n] = total.astype(BF16)

            send(sums.at[h, s2, pl.ds(0, top)], ra2.at[a], s_send.at[h], ra2_sem.at[a], up).start()
            send(sums.at[h, s2, pl.ds(top, rows - top)], rb2.at[a], s_send.at[h], rb2_sem.at[a], down).start()
            send(sums.at[h, sp, pl.ds(top, rows - top)], fl2.at[b, pl.ds(top, rows - top)], s_send.at[h], fl2_sem.at[b], up).start()
            send(sums.at[h, sm, pl.ds(0, top)], fr2.at[b, pl.ds(0, top)], s_send.at[h], fr2_sem.at[b], down).start()

            @pl.when(i + SLOTS < pieces)
            def _():
                pl.semaphore_signal(credit, inc=1, device_id=partner, device_id_type=MESH)

        @pl.when(t + 2 < pieces)
        def _():
            @pl.when(t + 2 >= SLOTS)
            def _():
                slot = (t + 2) % SLOTS
                wait_for(own.at[slot, pl.ds(0, last)], a_send.at[slot])
                wait_for(own.at[slot], par_send.at[slot])
                pl.semaphore_wait(credit, 1)

            load(t + 2)

        @pl.when(t < pieces)
        def _():
            load_state(t)

        @pl.when((t >= 3) & (t < pieces + 3))
        def _():
            i = t - 3
            h, a, b = i % HOLD, i % RING_A, i % RING_F
            wait_for(ra2.at[a], ra2_sem.at[a])
            wait_for(rb2.at[a], rb2_sem.at[a])
            sums[h, sp, pl.ds(0, top)] = (hold[h, sp, pl.ds(0, top)] + ra2[a].astype(F32)).astype(BF16)
            sums[h, sm, pl.ds(top, rows - top)] = (hold[h, sm, pl.ds(top, rows - top)] + rb2[a].astype(F32)).astype(BF16)
            send(sums.at[h, sp, pl.ds(0, top)], fl2.at[b, pl.ds(0, top)], s_send.at[h], fl2_sem.at[b], up).start()
            send(sums.at[h, sm, pl.ds(top, rows - top)], fr2.at[b, pl.ds(top, rows - top)], s_send.at[h], fr2_sem.at[b], down).start()

        @pl.when((t >= 4) & (t < pieces + 4))
        def _():
            i = t - 4
            h, b = i % HOLD, i % RING_F
            wait_for(fl2.at[b], fl2_sem.at[b])
            wait_for(fr2.at[b], fr2_sem.at[b])
            g[i, core] = (hold[h, s] + fl2[b].astype(F32) + fr2[b].astype(F32)).astype(BF16)
            send(g.at[i, core], g.at[i, core], g_send.at[i], g_sem.at[i], partner).start()
            wait_for(w_old.at[i], w_sem.at[i])

            def take(m, v):
                w_new[i] = adamw(w_old[i].astype(F32), m, v, g[i, core].astype(F32))[0]

            @pl.when(i < wide)
            def _():
                wait_for(mv_own.at[i], mv_sem.at[i])
                wait_for(mv_par.at[i], mp_sem.at[i])

                def both(n):
                    mine, other = mv_own[i, n, :, core, :], mv_par[i, n, :, core, :]
                    return jnp.concatenate([jnp.where(core == 0, mine, other), jnp.where(core == 0, other, mine)], 0)

                take(both(0), both(1))

            @pl.when(i >= wide)
            def _():
                q = i - wide

                @pl.when(q // half == core)
                def _():
                    wait_for(mv_down.at[q], mv_sem.at[i])

                @pl.when(q // half != core)
                def _():
                    wait_for(mv_down.at[q], mp_sem.at[i])

                take(mv_down[q, 0], mv_down[q, 1])

            def share(part):
                send(w_new.at[i], part(f, 0, rows), n_send.at[i], nl_sem.at[i], right).start()
                send(w_new.at[i], part(f, 0, rows), f_send.at[i], nr_sem.at[i], left).start()
                pltpu.make_async_copy(w_new.at[i], part(f, 0, rows), n_own.at[i]).start()

            unit(i, share)

        @pl.when(t >= 5)
        def _():
            i = t - 5

            @pl.when(i < pieces)
            def _():
                wait_for(w_new.at[i], nl_sem.at[i])
                wait_for(w_new.at[i], nr_sem.at[i])
                wait_for(w_new.at[i], n_send.at[i])
                wait_for(w_new.at[i], f_send.at[i])

                def forward(part):
                    low, high = part(fm, 0, top), part(fp, top, rows - top)
                    send(low, low, n_send.at[i], no_sem.at[i], right).start()
                    send(high, high, f_send.at[i], no_sem.at[i], left).start()

                unit(i, forward)

    @pl.loop(0, pieces)
    def _(i):
        wait_for(g.at[i, core], g_sem.at[i])
        pltpu.make_async_copy(g.at[i], out.at[i], out_sem.at[i]).start()

    for n in range(SLOTS):
        slot = (pieces + n) % SLOTS
        wait_for(own.at[slot, pl.ds(0, last)], a_send.at[slot])
        wait_for(own.at[slot], par_send.at[slot])
    for n in range(HOLD):
        wait_for(sums.at[n, pl.ds(0, last)], s_send.at[n])

    @pl.loop(0, pieces)
    def _(i):
        wait_for(g.at[i, core], g_send.at[i])
        wait_for(w_new.at[i], n_own.at[i])
        wait_for(w_new.at[i], no_sem.at[i])
        wait_for(w_new.at[i, pl.ds(0, top)], n_send.at[i])
        wait_for(w_new.at[i, pl.ds(top, rows - top)], f_send.at[i])

        @pl.when(i < wide)
        def _():
            wait_for(mv_par.at[i], mp_send.at[i])

        @pl.when((i >= wide) & ((i - wide) // half == core))
        def _():
            wait_for(mv_down.at[0], mp_send.at[i])

        pltpu.make_async_copy(g.at[i], out.at[i], out_sem.at[i]).wait()


def reduce_and_step(terms, weights, m, v, side):
    _, layers, d, ff = terms[0].shape
    quarters = ff // d
    rows, cols = d // (side * side), d
    pieces, wide = 3 * quarters, 2 * quarters
    if side != 4 or layers != 2 or quarters != 4:
        raise ValueError("wrong sizes")
    top = (rows // 2 + 7) // 8 * 8
    dma = pltpu.SemaphoreType.DMA
    any_ = pl.BlockSpec(memory_space=pl.ANY)
    own = m[0].shape[0]
    one = functools.partial(jax.ShapeDtypeStruct, dtype=BF16)
    return pl.pallas_call(
        functools.partial(reduce_kernel, side, quarters, rows, cols),
        out_shape=[
            one((pieces, layers, rows, cols)),
            one((side, rows, ff)),
            one((side, rows, ff)),
            one((side, rows * quarters // 2, d)),
            one((side, rows * quarters // 2, d)),
        ],
        in_specs=[any_] * 12,
        out_specs=[any_] * 5,
        scratch_shapes=[
            pltpu.VMEM((SLOTS, side, side, rows, cols), BF16),
            pltpu.VMEM((SLOTS, side, side, rows, cols), BF16),
            pltpu.VMEM((RING_A, side // 2, rows, cols), BF16),
            pltpu.VMEM((RING_A, side // 2, rows, cols), BF16),
            pltpu.VMEM((RING_F, side, rows, cols), BF16),
            pltpu.VMEM((RING_F, side, rows, cols), BF16),
            pltpu.VMEM((HOLD, side, rows, cols), F32),
            pltpu.VMEM((HOLD, side, rows, cols), BF16),
            pltpu.VMEM((RING_A, top, cols), BF16),
            pltpu.VMEM((RING_A, rows - top, cols), BF16),
            pltpu.VMEM((RING_F, rows, cols), BF16),
            pltpu.VMEM((RING_F, rows, cols), BF16),
            pltpu.VMEM((pieces, layers, rows, cols), BF16),
            pltpu.VMEM((wide, 2, own, layers, cols), F32),
            pltpu.VMEM((wide, 2, own, layers, cols), F32),
            pltpu.VMEM((quarters, 2, rows, cols), F32),
            pltpu.VMEM((pieces, rows, cols), BF16),
            pltpu.VMEM((pieces, rows, cols), BF16),
            *(dma((SLOTS,)) for _ in range(4)),
            *(dma((RING_A,)) for _ in range(2)),
            *(dma((RING_F,)) for _ in range(2)),
            dma((HOLD,)),
            *(dma((RING_A,)) for _ in range(2)),
            *(dma((RING_F,)) for _ in range(2)),
            *(dma((pieces,)) for _ in range(3)),
            *(dma((pieces,)) for _ in range(10)),
            pltpu.SemaphoreType.REGULAR,
        ],
        compiler_params=pltpu.CompilerParams(collective_id=0, has_side_effects=True, vmem_limit_bytes=67043328),
        name="reduce_and_step",
    )(*terms, *weights, *m, *v)


def moments_kernel(side, quarters, rows, cols, *refs):
    pieces_ref, ins, outs = refs[0], refs[1:7], refs[7:13]
    g, bufs, g_sem, in_sem, out_sem = refs[13], refs[14:20], *refs[20:]
    core = Place(side).core
    half = quarters // 2
    g_load = pltpu.make_async_copy(pieces_ref, g, g_sem)
    g_load.start()
    loads = [pltpu.make_async_copy(ref, buf, in_sem.at[n]) for n, (ref, buf) in enumerate(zip(ins, bufs, strict=True))]
    stores = [pltpu.make_async_copy(buf, ref, out_sem.at[n]) for n, (ref, buf) in enumerate(zip(outs, bufs, strict=True))]
    for one in loads:
        one.start()
    g_load.wait()
    for n in range(3):
        m, v = bufs[n], bufs[3 + n]
        loads[n].wait()
        loads[3 + n].wait()

        if n < 2:

            @pl.loop(0, quarters)
            def _(q, n=n, m=m, v=v):
                at = pl.ds(pl.multiple_of(q * cols, 128), cols)
                for layer in range(2):
                    whole = g[n * quarters + q, layer].astype(F32)
                    grad = jnp.where(core == 0, whole[: rows // 2], whole[rows // 2 :])
                    m[:, layer, at] = 0.9 * m[:, layer, at] + 0.1 * grad
                    v[:, layer, at] = 0.95 * v[:, layer, at] + 0.05 * grad * grad

        else:

            @pl.loop(0, half)
            def _(q, n=n, m=m, v=v):
                at = pl.ds(pl.multiple_of(q * rows, 8), rows)
                for layer in range(2):
                    grad = g[n * quarters + core * half + q, layer].astype(F32)
                    m[layer, at] = 0.9 * m[layer, at] + 0.1 * grad
                    v[layer, at] = 0.95 * v[layer, at] + 0.05 * grad * grad

        stores[n].start()
        stores[3 + n].start()
    for one in stores:
        one.wait()


def moments(pieces, m, v, side, quarters):
    arrays = [*m, *v]
    any_ = pl.BlockSpec(memory_space=pl.ANY)
    rows, cols = pieces.shape[2:]
    size = sum(one.size for one in arrays)
    dma = pltpu.SemaphoreType.DMA
    return pl.pallas_call(
        functools.partial(moments_kernel, side, quarters, rows, cols),
        out_shape=[jax.ShapeDtypeStruct(one.shape, F32) for one in arrays],
        in_specs=[any_] * 7,
        out_specs=[any_] * 6,
        scratch_shapes=[
            pltpu.VMEM(pieces.shape, BF16),
            *(pltpu.VMEM(one.shape, F32) for one in arrays),
            dma,
            dma((6,)),
            dma((6,)),
        ],
        cost_estimate=pl.CostEstimate(flops=16 * size, bytes_accessed=8 * size, transcendentals=0),
        compiler_params=pltpu.CompilerParams(vmem_limit_bytes=67043328),
        name="moments",
    )(pieces, *arrays)


def place_kernel(side, jobs, n_in, has_out, *refs):
    ins = refs[:n_in]
    out = refs[n_in + has_out]
    scratch = refs[n_in + has_out + 1 :]
    bufs, in_sem, out_sem = scratch[:n_in], scratch[n_in], scratch[n_in + 1]
    at = Place(side)
    loads = [pltpu.make_async_copy(ref, buf, in_sem.at[n]) for n, (ref, buf) in enumerate(zip(ins, bufs, strict=True))]
    for one in loads:
        one.start()
    stores = []
    for n, (partner, along, first, per_chip) in enumerate(jobs):
        loads[n].wait()
        for bf in range(side):
            if partner:
                chip, layer = bf * at.ms + (at.f + along) % side * at.mf, 1 - at.core
            else:
                chip, layer = bf * at.mf + (at.s + along) % side * at.ms, at.core
            start = pl.multiple_of(chip * per_chip + first, 8)
            stores.append(pltpu.make_async_copy(bufs[n].at[bf], out.at[layer, pl.ds(start, bufs[n].shape[1])], out_sem.at[n, bf]))
            stores[-1].start()
    for one in stores:
        one.wait()


def place(side, shape, out, jobs):
    ins = [job[0] for job in jobs]
    size = sum(one.size for one in ins)
    any_ = pl.BlockSpec(memory_space=pl.ANY)
    has_out = out is not None
    return pl.pallas_call(
        functools.partial(place_kernel, side, [job[1:] for job in jobs], len(ins), has_out),
        out_shape=jax.ShapeDtypeStruct(shape, BF16),
        in_specs=[any_] * (len(ins) + has_out),
        out_specs=any_,
        input_output_aliases={len(ins): 0} if has_out else {},
        scratch_shapes=[pltpu.VMEM(one.shape, BF16) for one in ins]
        + [pltpu.SemaphoreType.DMA((len(ins),)), pltpu.SemaphoreType.DMA((len(ins), side))],
        cost_estimate=pl.CostEstimate(flops=4 * size, bytes_accessed=4 * size, transcendentals=0),
        compiler_params=pltpu.CompilerParams(vmem_limit_bytes=67043328),
        name="place",
    )(*ins, *((out,) if has_out else ()))


def solution(mesh):
    dp = mesh.shape["dp"]
    side = math.isqrt(dp // 2)

    def along(step):
        pairs = []
        for n in range(dp):
            core, x, y = n % 2, n // 2 // side, n // 2 % side
            x, y = (x, (y + step) % side) if core == 0 else ((x + step) % side, y)
            pairs.append((n, (x * side + y) * 2 + core))
        return pairs

    up, down = along(1), along(side - 1)
    swap = [(n, n + 1 - 2 * (n % 2)) for n in range(dp)]

    def move(x, pairs):
        return lax.ppermute(x, "dp", pairs)

    def step(*arrays):
        terms, weights, m, v = (arrays[i : i + 3] for i in (0, 3, 6, 9))
        quarters = terms[0].shape[3] // terms[0].shape[2]
        m, v = ([one.transpose(1, 0, 2) if n < 2 else one for n, one in enumerate(which)] for which in (m, v))
        pieces, *units = reduce_and_step(terms, weights, m, v, side)

        below = [move(x, up) for x in units]
        above = [move(x, down) for x in units]
        across = [move((below, above)[n % 2][n], (up, down)[n % 2]) for n in range(4)]
        stages = [[(0, x) for x in units], [(side - 1, x) for x in below], [(1, x) for x in above], [(2, x) for x in across]]
        per_chip = [weights[n].shape[1] // (side * side) for n in range(3)]

        whole = []
        for n in range(3):
            out = None
            for group in ((0,), (1, 2), (3,)):
                jobs = []
                for stage in group:
                    for part in (n,) if n < 2 else (2, 3):
                        steps, x = stages[stage][part]
                        first = x.shape[1] * (part - 2) if n == 2 else 0
                        jobs.append((x, False, steps, first, per_chip[n]))
                        jobs.append((move(x, swap), True, steps, first, per_chip[n]))
                out = place(side, weights[n].shape, out, jobs)
            whole.append(out)

        new = moments(pieces, m, v, side, quarters)
        return (*whole, *(one.transpose(1, 0, 2) if n % 3 < 2 else one for n, one in enumerate(new)))

    all_of, cut = P(None, None, None), P(None, "dp", None)
    return jax.shard_map(
        step,
        mesh=mesh,
        in_specs=(P(("rep", "dp"), None, None, None),) * 3 + (all_of,) * 3 + (cut,) * 6,
        out_specs=(P("rep", None, None),) * 3 + (P("rep", "dp", None),) * 6,
        check_vma=False,
    )
```

```python
import functools
import math

import jax
import jax.numpy as jnp
from jax import lax
from jax.experimental import pallas as pl
from jax.experimental.pallas import tpu as pltpu
from jax.sharding import PartitionSpec as P


MESH = pl.DeviceIdType.MESH
F32, BF16 = jnp.float32, jnp.bfloat16
SLOTS = 4
HOLD = 3
RING_A, RING_F = 4, 6
AHEAD = (2, 1, 3, 0)
LATE = 4


def adamw(w, m, v, g):
    m = 0.9 * m + 0.1 * g
    v = 0.95 * v + 0.05 * g * g
    step = m * lax.rsqrt(v + 1e-8) + 0.1 * w
    return (w - 0.02 * step).astype(BF16), m, v


class Place:
    def __init__(self, side):
        me = lax.axis_index("dp")
        self.side = side
        self.core = me % 2
        chip = me // 2
        x, y = chip // side, chip % side
        self.chip = chip
        self.f = x + self.core * (y - x)
        self.s = y + self.core * (x - y)
        self.mf = side - (side - 1) * self.core
        self.ms = 1 + (side - 1) * self.core

    def device(self, df, ds):
        f, s = (self.f + df) % self.side, (self.s + ds) % self.side
        return {"dp": (f * self.mf + s * self.ms) * 2 + self.core}

    def partner(self):
        return {"dp": self.chip * 2 + 1 - self.core}

    def around(self):
        d = self.side - 1
        return [self.device(1, 0), self.device(d, 0), self.device(0, 1), self.device(0, d), self.partner()]

    def greet(self):
        barrier = pltpu.get_barrier_semaphore()
        others = self.around()
        for other in others:
            pl.semaphore_signal(barrier, inc=1, device_id=other, device_id_type=MESH)
        pl.semaphore_wait(barrier, len(others))


def send(src, dst, send_sem, recv_sem, device):
    return pltpu.make_async_remote_copy(
        src_ref=src, dst_ref=dst, send_sem=send_sem, recv_sem=recv_sem, device_id=device, device_id_type=MESH
    )


def wait_for(ref, sem):
    pltpu.make_async_copy(ref, ref, sem).wait()


def reduce_kernel(side, quarters, rows, cols, *refs):
    terms, weights, ms, vs = (refs[n : n + 3] for n in (0, 3, 6, 9))
    out, units = refs[12], refs[13:17]
    (own, par, ra, rb, fl, fr, hold, sums, ra2, rb2, fl2, fr2, g, mv_own, mv_par, mv_down, w_old, w_new) = refs[17:35]
    (own_sem, par_send, par_sem, a_send, ra_sem, rb_sem, fl_sem, fr_sem, s_send, ra2_sem, rb2_sem, fl2_sem, fr2_sem, g_send, g_sem, out_sem) = refs[35:51]
    (w_sem, mv_sem, mp_sem, mp_send, n_send, n_own, nl_sem, nr_sem, no_sem, f_send, credit) = refs[51:]
    pieces = 3 * quarters
    wide = 2 * quarters
    half = side // 2
    top = (rows // 2 + 7) // 8 * 8
    at = Place(side)
    core, f, s = at.core, at.f, at.s
    last = side - 1
    right, left = at.device(1, 0), at.device(last, 0)
    up, down = at.device(0, 1), at.device(0, last)
    partner = at.partner()
    fp, fm, f2 = (f + 1) % side, (f + last) % side, (f + 2) % side
    sp, sm, s2 = (s + 1) % side, (s + last) % side, (s + 2) % side
    at.greet()

    def columns(quarter):
        return pl.ds(pl.multiple_of(quarter * cols, 128), cols)

    def block(refs, which, lead, layer, quarter, chip):
        ref = refs[which]
        if which < 2:
            return ref.at[*lead, layer, pl.ds(pl.multiple_of(chip * rows, 8), rows), columns(quarter)]
        return ref.at[*lead, layer, pl.ds(pl.multiple_of((chip * quarters + quarter) * rows, 8), rows), :]

    def each(i, do):
        for which in range(3):

            @pl.when(i // quarters == which)
            def _(which=which):
                do(which, i % quarters)

    def load(i):
        slot = i % SLOTS

        def do(which, quarter):
            for ahead in AHEAD:

                @pl.loop(0, side)
                def _(n, ahead=ahead):
                    theirs, mine = (s + ahead) % side, (f + ahead) % side
                    send(
                        block(terms, which, (0,), 1 - core, quarter, theirs * at.ms + n * at.mf),
                        par.at[slot, theirs, n],
                        par_send.at[slot],
                        par_sem.at[slot, ahead],
                        partner,
                    ).start()
                    pltpu.make_async_copy(
                        block(terms, which, (0,), core, quarter, mine * at.mf + n * at.ms), own.at[slot, mine, n], own_sem.at[slot, ahead]
                    ).start()

        each(i, do)

    def load_state(i):
        def do(which, quarter):
            pltpu.make_async_copy(block(weights, which, (), core, quarter, at.chip), w_old.at[i], w_sem.at[i]).start()
            for n, ref in enumerate((ms[which], vs[which])):
                if which < 2:
                    part = ref.at[:, :, columns(quarter)]
                    pltpu.make_async_copy(part, mv_own.at[i, n], mv_sem.at[i]).start()
                    send(part, mv_par.at[i, n], mp_send.at[i], mp_sem.at[i], partner).start()
                else:

                    @pl.when(quarter // half == core)
                    def _(n=n, ref=ref):
                        here = pl.ds(pl.multiple_of(quarter % half * rows, 8), rows)
                        pltpu.make_async_copy(ref.at[core, here], mv_down.at[quarter, n], mv_sem.at[i]).start()
                        send(ref.at[1 - core, here], mv_down.at[quarter, n], mp_send.at[i], mp_sem.at[i], partner).start()

        each(i, do)

    def unit(i, do):
        for n in range(2):

            @pl.when(i // quarters == n)
            def _(n=n):
                do(lambda bf, at_row, size: units[n].at[bf, pl.ds(at_row, size), columns(i % quarters)])

        for n in range(2):

            @pl.when((i >= wide) & ((i - wide) // half == n))
            def _(n=n):
                start = pl.multiple_of(i % half * rows, 8)
                do(lambda bf, at_row, size: units[2 + n].at[bf, pl.ds(start + at_row, size), :])

    def pair(slot, bf, bs):
        return own[slot, bf, bs].astype(F32) + par[slot, bf, bs].astype(F32)

    def arrive(slot, ahead):
        wait_for(own.at[slot, 0], own_sem.at[slot, ahead])
        wait_for(par.at[slot, 0], par_sem.at[slot, ahead])

    def shared(t):
        n = t - 3 - LATE + jnp.maximum(t + 1 - pieces, 0)
        return jnp.clip(n, 0, jnp.minimum(jnp.maximum(t - 3, 0), pieces))

    load(0)
    load(1)

    @pl.loop(0, pieces + 5)
    def _(t):
        @pl.when(t < pieces)
        def _():
            i, slot = t, t % SLOTS
            a, b = i % RING_A, i % RING_F
            arrive(slot, 2)

            @pl.loop(0, side)
            def _(n):
                own[slot, f2, n] = pair(slot, f2, n).astype(BF16)

            send(own.at[slot, f2, pl.ds(0, half)], ra.at[a], a_send.at[slot], ra_sem.at[a], right).start()
            send(own.at[slot, f2, pl.ds(half, half)], rb.at[a], a_send.at[slot], rb_sem.at[a], left).start()

            arrive(slot, 1)
            arrive(slot, last)

            @pl.loop(0, half)
            def _(n):
                own[slot, fp, half + n] = pair(slot, fp, half + n).astype(BF16)
                own[slot, fm, n] = pair(slot, fm, n).astype(BF16)

            send(own.at[slot, fp, pl.ds(half, half)], fl.at[b, pl.ds(half, half)], a_send.at[slot], fl_sem.at[b], right).start()
            send(own.at[slot, fm, pl.ds(0, half)], fr.at[b, pl.ds(0, half)], a_send.at[slot], fr_sem.at[b], left).start()

        @pl.when((t >= 1) & (t < pieces + 1))
        def _():
            i = t - 1
            slot, a, b = i % SLOTS, i % RING_A, i % RING_F
            wait_for(ra.at[a], ra_sem.at[a])
            wait_for(rb.at[a], rb_sem.at[a])

            @pl.loop(0, half)
            def _(n):
                own[slot, fp, n] = (pair(slot, fp, n) + ra[a, n].astype(F32)).astype(BF16)
                own[slot, fm, half + n] = (pair(slot, fm, half + n) + rb[a, n].astype(F32)).astype(BF16)

            send(own.at[slot, fp, pl.ds(0, half)], fl.at[b, pl.ds(0, half)], a_send.at[slot], fl_sem.at[b], right).start()
            send(own.at[slot, fm, pl.ds(half, half)], fr.at[b, pl.ds(half, half)], a_send.at[slot], fr_sem.at[b], left).start()

        @pl.when((t >= 2) & (t < pieces + 2))
        def _():
            i = t - 2
            slot, h, a, b = i % SLOTS, i % HOLD, i % RING_A, i % RING_F

            @pl.when(i >= HOLD)
            def _():
                wait_for(sums.at[h, pl.ds(0, last)], s_send.at[h])

            arrive(slot, 0)
            wait_for(fl.at[b], fl_sem.at[b])
            wait_for(fr.at[b], fr_sem.at[b])

            @pl.loop(0, side)
            def _(n):
                total = pair(slot, f, n) + fl[b, n].astype(F32) + fr[b, n].astype(F32)
                hold[h, n] = total
                sums[h, n] = total.astype(BF16)

            send(sums.at[h, s2, pl.ds(0, top)], ra2.at[a], s_send.at[h], ra2_sem.at[a], up).start()
            send(sums.at[h, s2, pl.ds(top, rows - top)], rb2.at[a], s_send.at[h], rb2_sem.at[a], down).start()
            send(sums.at[h, sp, pl.ds(top, rows - top)], fl2.at[b, pl.ds(top, rows - top)], s_send.at[h], fl2_sem.at[b], up).start()
            send(sums.at[h, sm, pl.ds(0, top)], fr2.at[b, pl.ds(0, top)], s_send.at[h], fr2_sem.at[b], down).start()

            @pl.when(i + SLOTS < pieces)
            def _():
                pl.semaphore_signal(credit, inc=1, device_id=partner, device_id_type=MESH)

        @pl.when(t + 2 < pieces)
        def _():
            @pl.when(t + 2 >= SLOTS)
            def _():
                slot = (t + 2) % SLOTS
                wait_for(own.at[slot, pl.ds(0, last)], a_send.at[slot])
                wait_for(own.at[slot], par_send.at[slot])
                pl.semaphore_wait(credit, 1)

            load(t + 2)

        @pl.when(t < pieces)
        def _():
            load_state(t)

        @pl.when((t >= 3) & (t < pieces + 3))
        def _():
            i = t - 3
            h, a, b = i % HOLD, i % RING_A, i % RING_F
            wait_for(ra2.at[a], ra2_sem.at[a])
            wait_for(rb2.at[a], rb2_sem.at[a])
            sums[h, sp, pl.ds(0, top)] = (hold[h, sp, pl.ds(0, top)] + ra2[a].astype(F32)).astype(BF16)
            sums[h, sm, pl.ds(top, rows - top)] = (hold[h, sm, pl.ds(top, rows - top)] + rb2[a].astype(F32)).astype(BF16)
            send(sums.at[h, sp, pl.ds(0, top)], fl2.at[b, pl.ds(0, top)], s_send.at[h], fl2_sem.at[b], up).start()
            send(sums.at[h, sm, pl.ds(top, rows - top)], fr2.at[b, pl.ds(top, rows - top)], s_send.at[h], fr2_sem.at[b], down).start()

        @pl.when((t >= 4) & (t < pieces + 4))
        def _():
            i = t - 4
            h, b = i % HOLD, i % RING_F
            wait_for(fl2.at[b], fl2_sem.at[b])
            wait_for(fr2.at[b], fr2_sem.at[b])
            g[i, core] = (hold[h, s] + fl2[b].astype(F32) + fr2[b].astype(F32)).astype(BF16)
            send(g.at[i, core], g.at[i, core], g_send.at[i], g_sem.at[i], partner).start()
            wait_for(w_old.at[i], w_sem.at[i])

            def take(m, v):
                w_new[i] = adamw(w_old[i].astype(F32), m, v, g[i, core].astype(F32))[0]

            @pl.when(i < wide)
            def _():
                wait_for(mv_own.at[i], mv_sem.at[i])
                wait_for(mv_par.at[i], mp_sem.at[i])

                def both(n):
                    mine, other = mv_own[i, n, :, core, :], mv_par[i, n, :, core, :]
                    return jnp.concatenate([jnp.where(core == 0, mine, other), jnp.where(core == 0, other, mine)], 0)

                take(both(0), both(1))

            @pl.when(i >= wide)
            def _():
                q = i - wide

                @pl.when(q // half == core)
                def _():
                    wait_for(mv_down.at[q], mv_sem.at[i])

                @pl.when(q // half != core)
                def _():
                    wait_for(mv_down.at[q], mp_sem.at[i])

                take(mv_down[q, 0], mv_down[q, 1])

        @pl.loop(shared(t - 1), shared(t))
        def _(i):
            def share(part):
                send(w_new.at[i], part(f, 0, rows), n_send.at[i], nl_sem.at[i], right).start()
                send(w_new.at[i], part(f, 0, rows), f_send.at[i], nr_sem.at[i], left).start()
                pltpu.make_async_copy(w_new.at[i], part(f, 0, rows), n_own.at[i]).start()

            unit(i, share)

        @pl.loop(shared(t - 2), shared(t - 1))
        def _(i):
            wait_for(w_new.at[i], nl_sem.at[i])
            wait_for(w_new.at[i], nr_sem.at[i])
            wait_for(w_new.at[i], n_send.at[i])
            wait_for(w_new.at[i], f_send.at[i])

            def forward(part):
                low, high = part(fm, 0, top), part(fp, top, rows - top)
                send(low, low, n_send.at[i], no_sem.at[i], right).start()
                send(high, high, f_send.at[i], no_sem.at[i], left).start()

            unit(i, forward)

    @pl.loop(0, pieces)
    def _(i):
        wait_for(g.at[i, core], g_sem.at[i])
        pltpu.make_async_copy(g.at[i], out.at[i], out_sem.at[i]).start()

    for n in range(SLOTS):
        slot = (pieces + n) % SLOTS
        wait_for(own.at[slot, pl.ds(0, last)], a_send.at[slot])
        wait_for(own.at[slot], par_send.at[slot])
    for n in range(HOLD):
        wait_for(sums.at[n, pl.ds(0, last)], s_send.at[n])

    @pl.loop(0, pieces)
    def _(i):
        wait_for(g.at[i, core], g_send.at[i])
        wait_for(w_new.at[i], n_own.at[i])
        wait_for(w_new.at[i], no_sem.at[i])
        wait_for(w_new.at[i, pl.ds(0, top)], n_send.at[i])
        wait_for(w_new.at[i, pl.ds(top, rows - top)], f_send.at[i])

        @pl.when(i < wide)
        def _():
            wait_for(mv_par.at[i], mp_send.at[i])

        @pl.when((i >= wide) & ((i - wide) // half == core))
        def _():
            wait_for(mv_down.at[0], mp_send.at[i])

        pltpu.make_async_copy(g.at[i], out.at[i], out_sem.at[i]).wait()


def reduce_and_step(terms, weights, m, v, side):
    _, layers, d, ff = terms[0].shape
    quarters = ff // d
    rows, cols = d // (side * side), d
    pieces, wide = 3 * quarters, 2 * quarters
    if side != 4 or layers != 2 or quarters != 4:
        raise ValueError("wrong sizes")
    top = (rows // 2 + 7) // 8 * 8
    dma = pltpu.SemaphoreType.DMA
    any_ = pl.BlockSpec(memory_space=pl.ANY)
    own = m[0].shape[0]
    one = functools.partial(jax.ShapeDtypeStruct, dtype=BF16)
    return pl.pallas_call(
        functools.partial(reduce_kernel, side, quarters, rows, cols),
        out_shape=[
            one((pieces, layers, rows, cols)),
            one((side, rows, ff)),
            one((side, rows, ff)),
            one((side, rows * quarters // 2, d)),
            one((side, rows * quarters // 2, d)),
        ],
        in_specs=[any_] * 12,
        out_specs=[any_] * 5,
        scratch_shapes=[
            pltpu.VMEM((SLOTS, side, side, rows, cols), BF16),
            pltpu.VMEM((SLOTS, side, side, rows, cols), BF16),
            pltpu.VMEM((RING_A, side // 2, rows, cols), BF16),
            pltpu.VMEM((RING_A, side // 2, rows, cols), BF16),
            pltpu.VMEM((RING_F, side, rows, cols), BF16),
            pltpu.VMEM((RING_F, side, rows, cols), BF16),
            pltpu.VMEM((HOLD, side, rows, cols), F32),
            pltpu.VMEM((HOLD, side, rows, cols), BF16),
            pltpu.VMEM((RING_A, top, cols), BF16),
            pltpu.VMEM((RING_A, rows - top, cols), BF16),
            pltpu.VMEM((RING_F, rows, cols), BF16),
            pltpu.VMEM((RING_F, rows, cols), BF16),
            pltpu.VMEM((pieces, layers, rows, cols), BF16),
            pltpu.VMEM((wide, 2, own, layers, cols), F32),
            pltpu.VMEM((wide, 2, own, layers, cols), F32),
            pltpu.VMEM((quarters, 2, rows, cols), F32),
            pltpu.VMEM((pieces, rows, cols), BF16),
            pltpu.VMEM((pieces, rows, cols), BF16),
            dma((SLOTS, side)),
            dma((SLOTS,)),
            dma((SLOTS, side)),
            dma((SLOTS,)),
            *(dma((RING_A,)) for _ in range(2)),
            *(dma((RING_F,)) for _ in range(2)),
            dma((HOLD,)),
            *(dma((RING_A,)) for _ in range(2)),
            *(dma((RING_F,)) for _ in range(2)),
            *(dma((pieces,)) for _ in range(3)),
            *(dma((pieces,)) for _ in range(10)),
            pltpu.SemaphoreType.REGULAR,
        ],
        compiler_params=pltpu.CompilerParams(collective_id=0, has_side_effects=True, vmem_limit_bytes=67043328),
        name="reduce_and_step",
    )(*terms, *weights, *m, *v)


def moments_kernel(side, quarters, rows, cols, *refs):
    pieces_ref, ins, outs = refs[0], refs[1:7], refs[7:13]
    g, bufs, g_sem, in_sem, out_sem = refs[13], refs[14:20], *refs[20:]
    core = Place(side).core
    half = quarters // 2
    g_load = pltpu.make_async_copy(pieces_ref, g, g_sem)
    g_load.start()
    loads = [pltpu.make_async_copy(ref, buf, in_sem.at[n]) for n, (ref, buf) in enumerate(zip(ins, bufs, strict=True))]
    stores = [pltpu.make_async_copy(buf, ref, out_sem.at[n]) for n, (ref, buf) in enumerate(zip(outs, bufs, strict=True))]
    for one in loads:
        one.start()
    g_load.wait()
    for n in range(3):
        m, v = bufs[n], bufs[3 + n]
        loads[n].wait()
        loads[3 + n].wait()

        if n < 2:

            @pl.loop(0, quarters)
            def _(q, n=n, m=m, v=v):
                at = pl.ds(pl.multiple_of(q * cols, 128), cols)
                for layer in range(2):
                    whole = g[n * quarters + q, layer].astype(F32)
                    grad = jnp.where(core == 0, whole[: rows // 2], whole[rows // 2 :])
                    m[:, layer, at] = 0.9 * m[:, layer, at] + 0.1 * grad
                    v[:, layer, at] = 0.95 * v[:, layer, at] + 0.05 * grad * grad

        else:

            @pl.loop(0, half)
            def _(q, n=n, m=m, v=v):
                at = pl.ds(pl.multiple_of(q * rows, 8), rows)
                for layer in range(2):
                    grad = g[n * quarters + core * half + q, layer].astype(F32)
                    m[layer, at] = 0.9 * m[layer, at] + 0.1 * grad
                    v[layer, at] = 0.95 * v[layer, at] + 0.05 * grad * grad

        stores[n].start()
        stores[3 + n].start()
    for one in stores:
        one.wait()


def moments(pieces, m, v, side, quarters):
    arrays = [*m, *v]
    any_ = pl.BlockSpec(memory_space=pl.ANY)
    rows, cols = pieces.shape[2:]
    size = sum(one.size for one in arrays)
    dma = pltpu.SemaphoreType.DMA
    return pl.pallas_call(
        functools.partial(moments_kernel, side, quarters, rows, cols),
        out_shape=[jax.ShapeDtypeStruct(one.shape, F32) for one in arrays],
        in_specs=[any_] * 7,
        out_specs=[any_] * 6,
        scratch_shapes=[
            pltpu.VMEM(pieces.shape, BF16),
            *(pltpu.VMEM(one.shape, F32) for one in arrays),
            dma,
            dma((6,)),
            dma((6,)),
        ],
        cost_estimate=pl.CostEstimate(flops=16 * size, bytes_accessed=8 * size, transcendentals=0),
        compiler_params=pltpu.CompilerParams(vmem_limit_bytes=67043328),
        name="moments",
    )(pieces, *arrays)


def place_kernel(side, jobs, n_in, has_out, *refs):
    ins = refs[:n_in]
    out = refs[n_in + has_out]
    scratch = refs[n_in + has_out + 1 :]
    bufs, in_sem, out_sem = scratch[:n_in], scratch[n_in], scratch[n_in + 1]
    at = Place(side)
    loads = [pltpu.make_async_copy(ref, buf, in_sem.at[n]) for n, (ref, buf) in enumerate(zip(ins, bufs, strict=True))]
    for one in loads:
        one.start()
    stores = []
    for n, (partner, along, first, per_chip) in enumerate(jobs):
        loads[n].wait()
        for bf in range(side):
            if partner:
                chip, layer = bf * at.ms + (at.f + along) % side * at.mf, 1 - at.core
            else:
                chip, layer = bf * at.mf + (at.s + along) % side * at.ms, at.core
            start = pl.multiple_of(chip * per_chip + first, 8)
            stores.append(pltpu.make_async_copy(bufs[n].at[bf], out.at[layer, pl.ds(start, bufs[n].shape[1])], out_sem.at[n, bf]))
            stores[-1].start()
    for one in stores:
        one.wait()


def place(side, shape, out, jobs):
    ins = [job[0] for job in jobs]
    size = sum(one.size for one in ins)
    any_ = pl.BlockSpec(memory_space=pl.ANY)
    has_out = out is not None
    return pl.pallas_call(
        functools.partial(place_kernel, side, [job[1:] for job in jobs], len(ins), has_out),
        out_shape=jax.ShapeDtypeStruct(shape, BF16),
        in_specs=[any_] * (len(ins) + has_out),
        out_specs=any_,
        input_output_aliases={len(ins): 0} if has_out else {},
        scratch_shapes=[pltpu.VMEM(one.shape, BF16) for one in ins]
        + [pltpu.SemaphoreType.DMA((len(ins),)), pltpu.SemaphoreType.DMA((len(ins), side))],
        cost_estimate=pl.CostEstimate(flops=4 * size, bytes_accessed=4 * size, transcendentals=0),
        compiler_params=pltpu.CompilerParams(vmem_limit_bytes=67043328),
        name="place",
    )(*ins, *((out,) if has_out else ()))


def solution(mesh):
    dp = mesh.shape["dp"]
    side = math.isqrt(dp // 2)

    def along(step):
        pairs = []
        for n in range(dp):
            core, x, y = n % 2, n // 2 // side, n // 2 % side
            x, y = (x, (y + step) % side) if core == 0 else ((x + step) % side, y)
            pairs.append((n, (x * side + y) * 2 + core))
        return pairs

    up, down = along(1), along(side - 1)
    swap = [(n, n + 1 - 2 * (n % 2)) for n in range(dp)]

    def move(x, pairs):
        return lax.ppermute(x, "dp", pairs)

    def step(*arrays):
        terms, weights, m, v = (arrays[i : i + 3] for i in (0, 3, 6, 9))
        quarters = terms[0].shape[3] // terms[0].shape[2]
        m, v = ([one.transpose(1, 0, 2) if n < 2 else one for n, one in enumerate(which)] for which in (m, v))
        pieces, *units = reduce_and_step(terms, weights, m, v, side)

        below = [move(x, up) for x in units]
        above = [move(x, down) for x in units]
        across = [move((below, above)[n % 2][n], (up, down)[n % 2]) for n in range(4)]
        stages = [[(0, x) for x in units], [(side - 1, x) for x in below], [(1, x) for x in above], [(2, x) for x in across]]
        per_chip = [weights[n].shape[1] // (side * side) for n in range(3)]

        whole = []
        for n in range(3):
            out = None
            for when, group in enumerate(((0,), (1, 2), (3,))):
                here, there = [], []
                for stage in group:
                    for part in (n,) if n < 2 else (2, 3):
                        steps, x = stages[stage][part]
                        first = x.shape[1] * (part - 2) if n == 2 else 0
                        here.append((x, False, steps, first, per_chip[n]))
                        there.append((move(x, swap), True, steps, first, per_chip[n]))
                if (when, n) == (2, 2):
                    out = place(side, weights[n].shape, out, here)
                    here = []
                out = place(side, weights[n].shape, out, here + there)
            whole.append(out)

        new = moments(pieces, m, v, side, quarters)
        return (*whole, *(one.transpose(1, 0, 2) if n % 3 < 2 else one for n, one in enumerate(new)))

    all_of, cut = P(None, None, None), P(None, "dp", None)
    return jax.shard_map(
        step,
        mesh=mesh,
        in_specs=(P(("rep", "dp"), None, None, None),) * 3 + (all_of,) * 3 + (cut,) * 6,
        out_specs=(P("rep", None, None),) * 3 + (P("rep", "dp", None),) * 6,
        check_vma=False,
    )
```

```python
import functools
import math

import jax
import jax.numpy as jnp
from jax import lax
from jax.experimental import pallas as pl
from jax.experimental.pallas import tpu as pltpu
from jax.sharding import PartitionSpec as P


MESH = pl.DeviceIdType.MESH
F32, BF16 = jnp.float32, jnp.bfloat16
SLOTS = 4
HOLD = 3
RING_A, RING_F = 4, 6
AHEAD = (2, 1, 3, 0)
LATE = 4


def adamw(w, m, v, g):
    m = 0.9 * m + 0.1 * g
    v = 0.95 * v + 0.05 * g * g
    step = m * lax.rsqrt(v + 1e-8) + 0.1 * w
    return (w - 0.02 * step).astype(BF16), m, v


class Place:
    def __init__(self, side):
        me = lax.axis_index("dp")
        self.side = side
        self.core = me % 2
        chip = me // 2
        x, y = chip // side, chip % side
        self.chip = chip
        self.f = x + self.core * (y - x)
        self.s = y + self.core * (x - y)
        self.mf = side - (side - 1) * self.core
        self.ms = 1 + (side - 1) * self.core

    def device(self, df, ds):
        f, s = (self.f + df) % self.side, (self.s + ds) % self.side
        return {"dp": (f * self.mf + s * self.ms) * 2 + self.core}

    def partner(self):
        return {"dp": self.chip * 2 + 1 - self.core}

    def around(self):
        d = self.side - 1
        return [self.device(1, 0), self.device(d, 0), self.device(0, 1), self.device(0, d), self.partner()]

    def greet(self):
        barrier = pltpu.get_barrier_semaphore()
        others = self.around()
        for other in others:
            pl.semaphore_signal(barrier, inc=1, device_id=other, device_id_type=MESH)
        pl.semaphore_wait(barrier, len(others))


def send(src, dst, send_sem, recv_sem, device):
    return pltpu.make_async_remote_copy(
        src_ref=src, dst_ref=dst, send_sem=send_sem, recv_sem=recv_sem, device_id=device, device_id_type=MESH
    )


def wait_for(ref, sem):
    pltpu.make_async_copy(ref, ref, sem).wait()


def reduce_kernel(side, quarters, rows, cols, *refs):
    terms, weights, ms, vs = (refs[n : n + 3] for n in (0, 3, 6, 9))
    out, units = refs[12], refs[13:17]
    (own, par, ra, rb, fl, fr, hold, sums, ra2, rb2, fl2, fr2, g, mv_own, mv_par, mv_down, w_old, w_new) = refs[17:35]
    (own_sem, par_send, par_sem, a_send, ra_sem, rb_sem, fl_sem, fr_sem, s_send, ra2_sem, rb2_sem, fl2_sem, fr2_sem, g_send, g_sem, out_sem) = refs[35:51]
    (w_sem, mv_sem, mp_sem, mp_send, n_send, n_own, nl_sem, nr_sem, no_sem, f_send, credit) = refs[51:]
    pieces = 3 * quarters
    wide = 2 * quarters
    half = side // 2
    top = (rows // 2 + 7) // 8 * 8
    at = Place(side)
    core, f, s = at.core, at.f, at.s
    last = side - 1
    right, left = at.device(1, 0), at.device(last, 0)
    up, down = at.device(0, 1), at.device(0, last)
    partner = at.partner()
    fp, fm, f2 = (f + 1) % side, (f + last) % side, (f + 2) % side
    sp, sm, s2 = (s + 1) % side, (s + last) % side, (s + 2) % side
    at.greet()

    def columns(quarter):
        return pl.ds(pl.multiple_of(quarter * cols, 128), cols)

    def block(refs, which, lead, layer, quarter, chip):
        ref = refs[which]
        if which < 2:
            return ref.at[*lead, layer, pl.ds(pl.multiple_of(chip * rows, 8), rows), columns(quarter)]
        return ref.at[*lead, layer, pl.ds(pl.multiple_of((chip * quarters + quarter) * rows, 8), rows), :]

    def each(i, do):
        for which in range(3):

            @pl.when(i // quarters == which)
            def _(which=which):
                do(which, i % quarters)

    def load(i):
        slot = i % SLOTS

        def do(which, quarter):
            for ahead in AHEAD:

                @pl.loop(0, side)
                def _(n, ahead=ahead):
                    theirs, mine = (s + ahead) % side, (f + ahead) % side
                    send(
                        block(terms, which, (0,), 1 - core, quarter, theirs * at.ms + n * at.mf),
                        par.at[slot, theirs, n],
                        par_send.at[slot],
                        par_sem.at[slot, ahead],
                        partner,
                    ).start()
                    pltpu.make_async_copy(
                        block(terms, which, (0,), core, quarter, mine * at.mf + n * at.ms), own.at[slot, mine, n], own_sem.at[slot, ahead]
                    ).start()

        each(i, do)

    def load_state(i):
        def do(which, quarter):
            pltpu.make_async_copy(block(weights, which, (), core, quarter, at.chip), w_old.at[i], w_sem.at[i]).start()
            for n, ref in enumerate((ms[which], vs[which])):
                if which < 2:
                    part = ref.at[:, :, columns(quarter)]
                    pltpu.make_async_copy(part, mv_own.at[i, n], mv_sem.at[i]).start()
                    send(part, mv_par.at[i, n], mp_send.at[i], mp_sem.at[i], partner).start()
                else:

                    @pl.when(quarter // half == core)
                    def _(n=n, ref=ref):
                        here = pl.ds(pl.multiple_of(quarter % half * rows, 8), rows)
                        pltpu.make_async_copy(ref.at[core, here], mv_down.at[quarter, n], mv_sem.at[i]).start()
                        send(ref.at[1 - core, here], mv_down.at[quarter, n], mp_send.at[i], mp_sem.at[i], partner).start()

        each(i, do)

    def unit(i, do):
        for n in range(2):

            @pl.when(i // quarters == n)
            def _(n=n):
                do(lambda bf, at_row, size: units[n].at[bf, pl.ds(at_row, size), columns(i % quarters)])

        for n in range(2):

            @pl.when((i >= wide) & ((i - wide) // half == n))
            def _(n=n):
                start = pl.multiple_of(i % half * rows, 8)
                do(lambda bf, at_row, size: units[2 + n].at[bf, pl.ds(start + at_row, size), :])

    def pair(slot, bf, bs):
        return own[slot, bf, bs].astype(F32) + par[slot, bf, bs].astype(F32)

    def arrive(slot, ahead):
        wait_for(own.at[slot, 0], own_sem.at[slot, ahead])
        wait_for(par.at[slot, 0], par_sem.at[slot, ahead])

    def shared(t):
        n = t - 3 - LATE + jnp.maximum(t + 1 - pieces, 0)
        return jnp.clip(n, 0, jnp.minimum(jnp.maximum(t - 3, 0), pieces))

    load(0)
    load(1)

    @pl.loop(0, pieces + 5)
    def _(t):
        @pl.when(t < pieces)
        def _():
            i, slot = t, t % SLOTS
            a, b = i % RING_A, i % RING_F
            arrive(slot, 2)

            @pl.loop(0, side)
            def _(n):
                own[slot, f2, n] = pair(slot, f2, n).astype(BF16)

            send(own.at[slot, f2, pl.ds(0, half)], ra.at[a], a_send.at[slot], ra_sem.at[a], right).start()
            send(own.at[slot, f2, pl.ds(half, half)], rb.at[a], a_send.at[slot], rb_sem.at[a], left).start()

            arrive(slot, 1)
            arrive(slot, last)

            @pl.loop(0, half)
            def _(n):
                own[slot, fp, half + n] = pair(slot, fp, half + n).astype(BF16)
                own[slot, fm, n] = pair(slot, fm, n).astype(BF16)

            send(own.at[slot, fp, pl.ds(half, half)], fl.at[b, pl.ds(half, half)], a_send.at[slot], fl_sem.at[b], right).start()
            send(own.at[slot, fm, pl.ds(0, half)], fr.at[b, pl.ds(0, half)], a_send.at[slot], fr_sem.at[b], left).start()

        @pl.when((t >= 1) & (t < pieces + 1))
        def _():
            i = t - 1
            slot, a, b = i % SLOTS, i % RING_A, i % RING_F
            wait_for(ra.at[a], ra_sem.at[a])
            wait_for(rb.at[a], rb_sem.at[a])

            @pl.loop(0, half)
            def _(n):
                own[slot, fp, n] = (pair(slot, fp, n) + ra[a, n].astype(F32)).astype(BF16)
                own[slot, fm, half + n] = (pair(slot, fm, half + n) + rb[a, n].astype(F32)).astype(BF16)

            send(own.at[slot, fp, pl.ds(0, half)], fl.at[b, pl.ds(0, half)], a_send.at[slot], fl_sem.at[b], right).start()
            send(own.at[slot, fm, pl.ds(half, half)], fr.at[b, pl.ds(half, half)], a_send.at[slot], fr_sem.at[b], left).start()

        @pl.when((t >= 2) & (t < pieces + 2))
        def _():
            i = t - 2
            slot, h, a, b = i % SLOTS, i % HOLD, i % RING_A, i % RING_F

            @pl.when(i >= HOLD)
            def _():
                wait_for(sums.at[h, pl.ds(0, last)], s_send.at[h])

            arrive(slot, 0)
            wait_for(fl.at[b], fl_sem.at[b])
            wait_for(fr.at[b], fr_sem.at[b])

            @pl.loop(0, side)
            def _(n):
                total = pair(slot, f, n) + fl[b, n].astype(F32) + fr[b, n].astype(F32)
                hold[h, n] = total
                sums[h, n] = total.astype(BF16)

            send(sums.at[h, s2, pl.ds(0, top)], ra2.at[a], s_send.at[h], ra2_sem.at[a], up).start()
            send(sums.at[h, s2, pl.ds(top, rows - top)], rb2.at[a], s_send.at[h], rb2_sem.at[a], down).start()
            send(sums.at[h, sp, pl.ds(top, rows - top)], fl2.at[b, pl.ds(top, rows - top)], s_send.at[h], fl2_sem.at[b], up).start()
            send(sums.at[h, sm, pl.ds(0, top)], fr2.at[b, pl.ds(0, top)], s_send.at[h], fr2_sem.at[b], down).start()

            @pl.when(i + SLOTS < pieces)
            def _():
                pl.semaphore_signal(credit, inc=1, device_id=partner, device_id_type=MESH)

        @pl.when(t + 2 < pieces)
        def _():
            @pl.when(t + 2 >= SLOTS)
            def _():
                slot = (t + 2) % SLOTS
                wait_for(own.at[slot, pl.ds(0, last)], a_send.at[slot])
                wait_for(own.at[slot], par_send.at[slot])
                pl.semaphore_wait(credit, 1)

            load(t + 2)

        @pl.when(t < pieces)
        def _():
            load_state(t)

        @pl.when((t >= 3) & (t < pieces + 3))
        def _():
            i = t - 3
            h, a, b = i % HOLD, i % RING_A, i % RING_F
            wait_for(ra2.at[a], ra2_sem.at[a])
            wait_for(rb2.at[a], rb2_sem.at[a])
            sums[h, sp, pl.ds(0, top)] = (hold[h, sp, pl.ds(0, top)] + ra2[a].astype(F32)).astype(BF16)
            sums[h, sm, pl.ds(top, rows - top)] = (hold[h, sm, pl.ds(top, rows - top)] + rb2[a].astype(F32)).astype(BF16)
            send(sums.at[h, sp, pl.ds(0, top)], fl2.at[b, pl.ds(0, top)], s_send.at[h], fl2_sem.at[b], up).start()
            send(sums.at[h, sm, pl.ds(top, rows - top)], fr2.at[b, pl.ds(top, rows - top)], s_send.at[h], fr2_sem.at[b], down).start()

        @pl.when((t >= 4) & (t < pieces + 4))
        def _():
            i = t - 4
            h, b = i % HOLD, i % RING_F
            wait_for(fl2.at[b], fl2_sem.at[b])
            wait_for(fr2.at[b], fr2_sem.at[b])
            g[i, core] = (hold[h, s] + fl2[b].astype(F32) + fr2[b].astype(F32)).astype(BF16)
            send(g.at[i, core], g.at[i, core], g_send.at[i], g_sem.at[i], partner).start()
            wait_for(w_old.at[i], w_sem.at[i])

            def take(m, v):
                w_new[i] = adamw(w_old[i].astype(F32), m, v, g[i, core].astype(F32))[0]

            @pl.when(i < wide)
            def _():
                wait_for(mv_own.at[i], mv_sem.at[i])
                wait_for(mv_par.at[i], mp_sem.at[i])

                def both(n):
                    mine, other = mv_own[i, n, :, core, :], mv_par[i, n, :, core, :]
                    return jnp.concatenate([jnp.where(core == 0, mine, other), jnp.where(core == 0, other, mine)], 0)

                take(both(0), both(1))

            @pl.when(i >= wide)
            def _():
                q = i - wide

                @pl.when(q // half == core)
                def _():
                    wait_for(mv_down.at[q], mv_sem.at[i])

                @pl.when(q // half != core)
                def _():
                    wait_for(mv_down.at[q], mp_sem.at[i])

                take(mv_down[q, 0], mv_down[q, 1])

        @pl.loop(shared(t - 1), shared(t))
        def _(i):
            def share(part):
                send(w_new.at[i], part(f, 0, rows), n_send.at[i], nl_sem.at[i], right).start()
                send(w_new.at[i], part(f, 0, rows), f_send.at[i], nr_sem.at[i], left).start()
                pltpu.make_async_copy(w_new.at[i], part(f, 0, rows), n_own.at[i]).start()

            unit(i, share)

        @pl.loop(shared(t - 2), shared(t - 1))
        def _(i):
            wait_for(w_new.at[i], nl_sem.at[i])
            wait_for(w_new.at[i], nr_sem.at[i])
            wait_for(w_new.at[i], n_send.at[i])
            wait_for(w_new.at[i], f_send.at[i])

            def forward(part):
                low, high = part(fm, 0, rows - top), part(fp, rows - top, top)
                send(low, low, n_send.at[i], no_sem.at[i], right).start()
                send(high, high, f_send.at[i], no_sem.at[i], left).start()

            unit(i, forward)

    @pl.loop(0, pieces)
    def _(i):
        wait_for(g.at[i, core], g_sem.at[i])
        pltpu.make_async_copy(g.at[i], out.at[i], out_sem.at[i]).start()

    for n in range(SLOTS):
        slot = (pieces + n) % SLOTS
        wait_for(own.at[slot, pl.ds(0, last)], a_send.at[slot])
        wait_for(own.at[slot], par_send.at[slot])
    for n in range(HOLD):
        wait_for(sums.at[n, pl.ds(0, last)], s_send.at[n])

    @pl.loop(0, pieces)
    def _(i):
        wait_for(g.at[i, core], g_send.at[i])
        wait_for(w_new.at[i], n_own.at[i])
        wait_for(w_new.at[i], no_sem.at[i])
        wait_for(w_new.at[i, pl.ds(0, rows - top)], n_send.at[i])
        wait_for(w_new.at[i, pl.ds(0, top)], f_send.at[i])

        @pl.when(i < wide)
        def _():
            wait_for(mv_par.at[i], mp_send.at[i])

        @pl.when((i >= wide) & ((i - wide) // half == core))
        def _():
            wait_for(mv_down.at[0], mp_send.at[i])

        pltpu.make_async_copy(g.at[i], out.at[i], out_sem.at[i]).wait()


def reduce_and_step(terms, weights, m, v, side):
    _, layers, d, ff = terms[0].shape
    quarters = ff // d
    rows, cols = d // (side * side), d
    pieces, wide = 3 * quarters, 2 * quarters
    if side != 4 or layers != 2 or quarters != 4:
        raise ValueError("wrong sizes")
    top = (rows // 2 + 7) // 8 * 8
    dma = pltpu.SemaphoreType.DMA
    any_ = pl.BlockSpec(memory_space=pl.ANY)
    own = m[0].shape[0]
    one = functools.partial(jax.ShapeDtypeStruct, dtype=BF16)
    return pl.pallas_call(
        functools.partial(reduce_kernel, side, quarters, rows, cols),
        out_shape=[
            one((pieces, layers, rows, cols)),
            one((side, rows, ff)),
            one((side, rows, ff)),
            one((side, rows * quarters // 2, d)),
            one((side, rows * quarters // 2, d)),
        ],
        in_specs=[any_] * 12,
        out_specs=[any_] * 5,
        scratch_shapes=[
            pltpu.VMEM((SLOTS, side, side, rows, cols), BF16),
            pltpu.VMEM((SLOTS, side, side, rows, cols), BF16),
            pltpu.VMEM((RING_A, side // 2, rows, cols), BF16),
            pltpu.VMEM((RING_A, side // 2, rows, cols), BF16),
            pltpu.VMEM((RING_F, side, rows, cols), BF16),
            pltpu.VMEM((RING_F, side, rows, cols), BF16),
            pltpu.VMEM((HOLD, side, rows, cols), F32),
            pltpu.VMEM((HOLD, side, rows, cols), BF16),
            pltpu.VMEM((RING_A, top, cols), BF16),
            pltpu.VMEM((RING_A, rows - top, cols), BF16),
            pltpu.VMEM((RING_F, rows, cols), BF16),
            pltpu.VMEM((RING_F, rows, cols), BF16),
            pltpu.VMEM((pieces, layers, rows, cols), BF16),
            pltpu.VMEM((wide, 2, own, layers, cols), F32),
            pltpu.VMEM((wide, 2, own, layers, cols), F32),
            pltpu.VMEM((quarters, 2, rows, cols), F32),
            pltpu.VMEM((pieces, rows, cols), BF16),
            pltpu.VMEM((pieces, rows, cols), BF16),
            dma((SLOTS, side)),
            dma((SLOTS,)),
            dma((SLOTS, side)),
            dma((SLOTS,)),
            *(dma((RING_A,)) for _ in range(2)),
            *(dma((RING_F,)) for _ in range(2)),
            dma((HOLD,)),
            *(dma((RING_A,)) for _ in range(2)),
            *(dma((RING_F,)) for _ in range(2)),
            *(dma((pieces,)) for _ in range(3)),
            *(dma((pieces,)) for _ in range(10)),
            pltpu.SemaphoreType.REGULAR,
        ],
        compiler_params=pltpu.CompilerParams(collective_id=0, has_side_effects=True, vmem_limit_bytes=67043328),
        name="reduce_and_step",
    )(*terms, *weights, *m, *v)


def moments_kernel(side, quarters, rows, cols, *refs):
    pieces_ref, ins, outs = refs[0], refs[1:7], refs[7:13]
    g, bufs, g_sem, in_sem, out_sem = refs[13], refs[14:20], *refs[20:]
    core = Place(side).core
    half = quarters // 2
    g_load = pltpu.make_async_copy(pieces_ref, g, g_sem)
    g_load.start()
    loads = [pltpu.make_async_copy(ref, buf, in_sem.at[n]) for n, (ref, buf) in enumerate(zip(ins, bufs, strict=True))]
    stores = [pltpu.make_async_copy(buf, ref, out_sem.at[n]) for n, (ref, buf) in enumerate(zip(outs, bufs, strict=True))]
    for one in loads:
        one.start()
    g_load.wait()
    for n in range(3):
        m, v = bufs[n], bufs[3 + n]
        loads[n].wait()
        loads[3 + n].wait()

        if n < 2:

            @pl.loop(0, quarters)
            def _(q, n=n, m=m, v=v):
                at = pl.ds(pl.multiple_of(q * cols, 128), cols)
                for layer in range(2):
                    whole = g[n * quarters + q, layer].astype(F32)
                    grad = jnp.where(core == 0, whole[: rows // 2], whole[rows // 2 :])
                    m[:, layer, at] = 0.9 * m[:, layer, at] + 0.1 * grad
                    v[:, layer, at] = 0.95 * v[:, layer, at] + 0.05 * grad * grad

        else:

            @pl.loop(0, half)
            def _(q, n=n, m=m, v=v):
                at = pl.ds(pl.multiple_of(q * rows, 8), rows)
                for layer in range(2):
                    grad = g[n * quarters + core * half + q, layer].astype(F32)
                    m[layer, at] = 0.9 * m[layer, at] + 0.1 * grad
                    v[layer, at] = 0.95 * v[layer, at] + 0.05 * grad * grad

        stores[n].start()
        stores[3 + n].start()
    for one in stores:
        one.wait()


def moments(pieces, m, v, side, quarters):
    arrays = [*m, *v]
    any_ = pl.BlockSpec(memory_space=pl.ANY)
    rows, cols = pieces.shape[2:]
    size = sum(one.size for one in arrays)
    dma = pltpu.SemaphoreType.DMA
    return pl.pallas_call(
        functools.partial(moments_kernel, side, quarters, rows, cols),
        out_shape=[jax.ShapeDtypeStruct(one.shape, F32) for one in arrays],
        in_specs=[any_] * 7,
        out_specs=[any_] * 6,
        scratch_shapes=[
            pltpu.VMEM(pieces.shape, BF16),
            *(pltpu.VMEM(one.shape, F32) for one in arrays),
            dma,
            dma((6,)),
            dma((6,)),
        ],
        cost_estimate=pl.CostEstimate(flops=16 * size, bytes_accessed=8 * size, transcendentals=0),
        compiler_params=pltpu.CompilerParams(vmem_limit_bytes=67043328),
        name="moments",
    )(pieces, *arrays)


def place_kernel(side, jobs, n_in, has_out, *refs):
    ins = refs[:n_in]
    out = refs[n_in + has_out]
    scratch = refs[n_in + has_out + 1 :]
    bufs, in_sem, out_sem = scratch[:n_in], scratch[n_in], scratch[n_in + 1]
    at = Place(side)
    loads = [pltpu.make_async_copy(ref, buf, in_sem.at[n]) for n, (ref, buf) in enumerate(zip(ins, bufs, strict=True))]
    for one in loads:
        one.start()
    stores = []
    for n, (partner, along, first, per_chip) in enumerate(jobs):
        loads[n].wait()
        for bf in range(side):
            if partner:
                chip, layer = bf * at.ms + (at.f + along) % side * at.mf, 1 - at.core
            else:
                chip, layer = bf * at.mf + (at.s + along) % side * at.ms, at.core
            start = pl.multiple_of(chip * per_chip + first, 8)
            stores.append(pltpu.make_async_copy(bufs[n].at[bf], out.at[layer, pl.ds(start, bufs[n].shape[1])], out_sem.at[n, bf]))
            stores[-1].start()
    for one in stores:
        one.wait()


def place(side, shape, out, jobs):
    ins = [job[0] for job in jobs]
    size = sum(one.size for one in ins)
    any_ = pl.BlockSpec(memory_space=pl.ANY)
    has_out = out is not None
    return pl.pallas_call(
        functools.partial(place_kernel, side, [job[1:] for job in jobs], len(ins), has_out),
        out_shape=jax.ShapeDtypeStruct(shape, BF16),
        in_specs=[any_] * (len(ins) + has_out),
        out_specs=any_,
        input_output_aliases={len(ins): 0} if has_out else {},
        scratch_shapes=[pltpu.VMEM(one.shape, BF16) for one in ins]
        + [pltpu.SemaphoreType.DMA((len(ins),)), pltpu.SemaphoreType.DMA((len(ins), side))],
        cost_estimate=pl.CostEstimate(flops=4 * size, bytes_accessed=4 * size, transcendentals=0),
        compiler_params=pltpu.CompilerParams(vmem_limit_bytes=67043328),
        name="place",
    )(*ins, *((out,) if has_out else ()))


def solution(mesh):
    dp = mesh.shape["dp"]
    side = math.isqrt(dp // 2)

    def along(step):
        pairs = []
        for n in range(dp):
            core, x, y = n % 2, n // 2 // side, n // 2 % side
            x, y = (x, (y + step) % side) if core == 0 else ((x + step) % side, y)
            pairs.append((n, (x * side + y) * 2 + core))
        return pairs

    up, down = along(1), along(side - 1)
    swap = [(n, n + 1 - 2 * (n % 2)) for n in range(dp)]

    def move(x, pairs):
        return lax.ppermute(x, "dp", pairs)

    def step(*arrays):
        terms, weights, m, v = (arrays[i : i + 3] for i in (0, 3, 6, 9))
        quarters = terms[0].shape[3] // terms[0].shape[2]
        m, v = ([one.transpose(1, 0, 2) if n < 2 else one for n, one in enumerate(which)] for which in (m, v))
        pieces, *units = reduce_and_step(terms, weights, m, v, side)

        below = [move(x, up) for x in units]
        above = [move(x, down) for x in units]
        across = [move((below, above)[n % 2][n], (up, down)[n % 2]) for n in range(4)]
        stages = [[(0, x) for x in units], [(side - 1, x) for x in below], [(1, x) for x in above], [(2, x) for x in across]]
        per_chip = [weights[n].shape[1] // (side * side) for n in range(3)]

        whole = []
        for n in range(3):
            out = None
            for when, group in enumerate(((0,), (1, 2), (3,))):
                here, there = [], []
                for stage in group:
                    for part in (n,) if n < 2 else (2, 3):
                        steps, x = stages[stage][part]
                        first = x.shape[1] * (part - 2) if n == 2 else 0
                        here.append((x, False, steps, first, per_chip[n]))
                        there.append((move(x, swap), True, steps, first, per_chip[n]))
                if (when, n) == (2, 2):
                    out = place(side, weights[n].shape, out, here)
                    here = []
                out = place(side, weights[n].shape, out, here + there)
            whole.append(out)

        new = moments(pieces, m, v, side, quarters)
        return (*whole, *(one.transpose(1, 0, 2) if n % 3 < 2 else one for n, one in enumerate(new)))

    all_of, cut = P(None, None, None), P(None, "dp", None)
    return jax.shard_map(
        step,
        mesh=mesh,
        in_specs=(P(("rep", "dp"), None, None, None),) * 3 + (all_of,) * 3 + (cut,) * 6,
        out_specs=(P("rep", None, None),) * 3 + (P("rep", "dp", None),) * 6,
        check_vma=False,
    )
```
